32 devices in a mesh: grp: 2 (over y), wide: 8 (over z, x), narrow: 2 (over core).
Axes of the slice: x: 2, y: 2, z: 4, core: 2. Of those that a mesh axis runs over, the one named last changes fastest.
Arguments:
- cache: bfloat16 [16, 48, 576], P('grp', ('wide', 'narrow')), parts along dimension 0, may hold values from -4 to 4
- lengths: int32 [16], P('grp'), parts along dimension 0, may hold values from 1 to 47, 128 in all
- slots: int32 [16], P('grp'), parts along dimension 0, may hold values from 0 to 7, each once
- query: bfloat16 [16, 1, 64, 576], P(('grp', 'wide'), None, 'narrow'), parts along dimension 0, may hold values from -200 to 200
Outputs:
- attended: bfloat16 [16, 1, 64, 512], P(('grp', 'wide'), None, 'narrow'), parts along dimension 0
The draws below stay inside these ranges and needn't reach their ends.
There are 2 independent parts, one for each index of `grp`. The reference program is written for one: setup_inputs(seed, part) draws one part's arguments, and reference() takes and returns one part's arrays. A program takes and returns all parts, laid end to end along the dimension named above; each array names one. Nothing has to cross between parts.
Inputs may be any that keep to these rules, and one draw needn't show every extreme that they name: `lengths`: each request has at most 47 cached positions, and some request has exactly that many in every draw; its 1 new tokens' entries follow its cached positions. `slots`: A permutation: every slot holds one request.
All inputs are finite; a program needn't handle non-finite values.
Results may differ from the reference program's by a relative error of at most 0.013.
Values may be sent and summed in bfloat16 or wider, within the bound.
A program may use at most 64 MiB of HBM per device.

```python
import math
import jax
import jax.numpy as jnp
import numpy as np
from jax import lax

HEAD_TOTAL = 64
LATENT_WIDTH = 512
ROTARY_WIDTH = 64
QUERY_TOKENS = 1
REQUEST_SLOTS = 8
CACHE_POSITIONS = 48


def draw_cache(key, part):
    array_shape = (REQUEST_SLOTS, CACHE_POSITIONS, LATENT_WIDTH + ROTARY_WIDTH)
    value_rows = jnp.clip(jax.random.normal(jax.random.fold_in(key, 3), array_shape, jnp.float32), -4.0, 4.0)
    return value_rows.astype(jnp.bfloat16)


def draw_query(key, part):
    array_shape = (REQUEST_SLOTS, QUERY_TOKENS, HEAD_TOTAL, LATENT_WIDTH + ROTARY_WIDTH)
    value_rows = jnp.clip(0.6 * jax.random.normal(jax.random.fold_in(key, 5), array_shape, jnp.float32), -2.4, 2.4)
    return value_rows.astype(jnp.bfloat16)


def length_profile(count, total, bound, skew):
    loads = [(1 << 20) // math.isqrt(rank ** skew) + 1 for rank in range(2, count + 1)]
    rest, holding = total - bound - (count - 1), [1] * (count - 1)
    while rest > 0:
        free = [i for i in range(count - 1) if holding[i] < bound]
        whole, budget = sum([loads[i] for i in free]), rest
        for i in free:
            extra = min(bound - holding[i], max(1, budget * loads[i] // whole), rest)
            holding[i] = holding[i] + extra
            rest = rest - extra
    return np.array([bound] + holding)


def ragged_sizes(key, count, total, reach, slope):
    if count == 2:
        one = jax.random.randint(key, (), max(1, total - reach), min(reach, total - 1) + 1)
        return jnp.stack([one, total - one])
    sizes = jnp.asarray(length_profile(count, total, reach, slope), jnp.int32)
    couples = (count - 1) // 2
    donor, sink = sizes[1:1 + 2 * couples:2], sizes[2:2 + 2 * couples:2]
    margin = jnp.minimum(donor - 1, reach - sink)
    shifted = jax.random.randint(jax.random.fold_in(key, 1), (couples,), 0, 1 << 20) % (margin + 1)
    sizes = sizes.at[1:1 + 2 * couples:2].set(donor - shifted).at[2:2 + 2 * couples:2].set(sink + shifted)
    return sizes[jax.random.permutation(jax.random.fold_in(key, 2), count)]


def setup_inputs(seed: int = 0, part: int = 0) -> dict:
    seeds = jax.random.split(jax.random.key(seed), 5)
    part_keys = jax.random.split(jax.random.fold_in(seeds[4], part), 5)
    return {
        "cache": draw_cache(jax.random.fold_in(jax.random.fold_in(seeds[4], part), 71), part),
        "lengths": ragged_sizes(part_keys[1], REQUEST_SLOTS, REQUEST_SLOTS * CACHE_POSITIONS // 3, CACHE_POSITIONS - QUERY_TOKENS, 2).astype(jnp.int32),
        "slots": jax.random.permutation(part_keys[2], REQUEST_SLOTS).astype(jnp.int32),
        "query": draw_query(jax.random.fold_in(jax.random.fold_in(seeds[4], part), 71), part),
    }


def reference(cache, lengths, slots, query):
    score_scale = 0.0721687836
    owner = jnp.argsort(slots).astype(jnp.int32)
    positions = jnp.arange(CACHE_POSITIONS, dtype=jnp.int32)
    forward_steps = jnp.arange(QUERY_TOKENS, dtype=jnp.int32)

    def attend(slot_index):
        request = owner[slot_index]
        cache_key_rows = cache[request].astype(jnp.float32)
        query_rows = query[slot_index].astype(jnp.float32)
        scores = jnp.einsum("thc,pc->thp", query_rows, cache_key_rows) * score_scale
        key_limit = lengths[request] + forward_steps + 1
        visible = positions[None, None, :] < key_limit[:, None, None]
        scores = jnp.where(visible, scores, -1.0e30)
        highest = jnp.max(scores, axis=2, keepdims=True)
        softmax_weights = jnp.where(visible, jnp.exp(scores - highest), 0.0)
        weight_sum = jnp.sum(softmax_weights, axis=2)
        rounded_length = lax.optimization_barrier(softmax_weights.astype(jnp.bfloat16)).astype(jnp.float32)
        latent_total = jnp.einsum("seg,gr->ser", rounded_length, cache_key_rows[:, :LATENT_WIDTH])
        return (latent_total / weight_sum[..., None]).astype(jnp.bfloat16)

    return lax.map(attend, jnp.arange(REQUEST_SLOTS, dtype=jnp.int32))
```

```python
import functools
import math

import jax
import jax.numpy as jnp
from jax import lax
from jax.experimental import pallas as pl
from jax.experimental.pallas import tpu as pltpu
from jax.sharding import PartitionSpec as P

LATENT_WIDTH = 512
UNROLL_LIMIT = 16

score_scale = 0.0721687836
floor_value = -1e30


def loop(count, body):
    if count <= UNROLL_LIMIT:
        for step in range(count):
            body(step)
    else:
        lax.fori_loop(0, count, lambda step, carry: (body(step), carry)[1], 0)


def owner_of(slot, slots_ref, request_count):
    if request_count <= UNROLL_LIMIT:
        owner = jnp.int32(0)
        for request in range(request_count):
            owner = jnp.where(slots_ref[request] == slot, jnp.int32(request), owner)
        return owner
    return lax.fori_loop(
        0,
        request_count,
        lambda request, owner: jnp.where(slots_ref[request] == slot, request, owner),
        jnp.int32(0),
    )


def kernel(
    wide_count,
    narrow_count,
    cache_hbm,
    lengths_hbm,
    slots_hbm,
    query_hbm,
    out_ref,
    cache_ref,
    lengths_ref,
    slots_ref,
    query_ref,
    outgoing,
    received,
    keys_ref,
    local_sem,
    send_sem,
    recv_sem,
):
    wide_index = lax.axis_index("wide")
    narrow_index = lax.axis_index("narrow")
    me = wide_index * narrow_count + narrow_index
    peer_count = wide_count * narrow_count
    request_count, shard_rows, channels = cache_ref.shape

    slots_copy = pltpu.make_async_copy(slots_hbm, slots_ref, local_sem.at[0])
    cache_copy = pltpu.make_async_copy(cache_hbm, cache_ref, local_sem.at[1])
    lengths_copy = pltpu.make_async_copy(lengths_hbm, lengths_ref, local_sem.at[2])
    query_copy = pltpu.make_async_copy(query_hbm, query_ref, local_sem.at[3])
    slots_copy.start()
    cache_copy.start()
    lengths_copy.start()
    query_copy.start()

    def peer(step):
        target = lax.rem(me + step + 1, peer_count)
        return lax.div(target, narrow_count), lax.rem(target, narrow_count)

    barrier = pltpu.get_barrier_semaphore()

    def greet(step):
        wide_peer, narrow_peer = peer(step)
        pl.semaphore_signal(
            barrier,
            inc=1,
            device_id={"wide": wide_peer, "narrow": narrow_peer},
            device_id_type=pl.DeviceIdType.MESH,
        )

    loop(peer_count - 1, greet)
    slots_copy.wait()
    cache_copy.wait()

    def order(slot):
        outgoing[slot] = cache_ref[owner_of(slot, slots_ref, request_count)]

    loop(request_count, order)
    own = owner_of(wide_index, slots_ref, request_count)
    received[me] = cache_ref[own]
    pl.semaphore_wait(barrier, peer_count - 1)

    def send(step):
        wide_peer, narrow_peer = peer(step)
        pltpu.make_async_remote_copy(
            src_ref=outgoing.at[wide_peer],
            dst_ref=received.at[me],
            send_sem=send_sem,
            recv_sem=recv_sem,
            device_id={"wide": wide_peer, "narrow": narrow_peer},
            device_id_type=pl.DeviceIdType.MESH,
        ).start()

    loop(peer_count - 1, send)
    lengths_copy.wait()
    query_copy.wait()
    own_length = lengths_ref[own]
    whole = received.at[pl.ds(0, peer_count - 1)]
    arrived = pltpu.make_async_copy(whole, whole, recv_sem)
    arrived.wait()

    bundle = 16 // math.gcd(16, shard_rows)

    def pack(step):
        rows = bundle * shard_rows
        first = step * bundle
        keys_ref[pl.ds(step * rows, rows), :] = jnp.concatenate(
            [received[first + i] for i in range(bundle)], axis=0
        )

    loop(peer_count // bundle, pack)
    keys = keys_ref[...]
    _, forward_steps, head_count, _ = query_ref.shape
    query_rows = query_ref[...].reshape(forward_steps * head_count, channels)
    scores = (
        lax.dot_general(
            query_rows, keys, (((1,), (1,)), ((), ())), preferred_element_type=jnp.float32
        )
        * score_scale
    )
    places = lax.broadcasted_iota(jnp.int32, scores.shape, 1)
    token = lax.broadcasted_iota(jnp.int32, scores.shape, 0) // head_count
    visible = places < own_length + 1 + token
    scores = jnp.where(visible, scores, floor_value)
    highest = jnp.max(scores, axis=1, keepdims=True)
    weights = jnp.where(visible, jnp.exp(scores - highest), 0.0)
    weight_sum = jnp.sum(weights, axis=1, keepdims=True)
    latent_total = jnp.dot(
        weights.astype(jnp.bfloat16), keys[:, :LATENT_WIDTH], preferred_element_type=jnp.float32
    )
    out_ref[...] = (latent_total / weight_sum).astype(jnp.bfloat16).reshape(out_ref.shape)
    pltpu.make_async_copy(whole, whole, send_sem).wait()


def shards(cache, lengths, slots, query):
    wide_count = lax.axis_size("wide")
    narrow_count = lax.axis_size("narrow")
    peer_count = wide_count * narrow_count
    request_count, shard_rows, channels = cache.shape
    _, forward_steps, head_count, _ = query.shape
    return pl.pallas_call(
        functools.partial(kernel, wide_count, narrow_count),
        out_shape=jax.ShapeDtypeStruct((1, forward_steps, head_count, LATENT_WIDTH), jnp.bfloat16),
        in_specs=[pl.BlockSpec(memory_space=pl.ANY)] * 4,
        out_specs=pl.BlockSpec(memory_space=pltpu.VMEM),
        scratch_shapes=[
            pltpu.VMEM(cache.shape, cache.dtype),
            pltpu.SMEM(lengths.shape, lengths.dtype),
            pltpu.SMEM(slots.shape, slots.dtype),
            pltpu.VMEM(query.shape, query.dtype),
            pltpu.VMEM(cache.shape, cache.dtype),
            pltpu.VMEM((peer_count, shard_rows, channels), cache.dtype),
            pltpu.VMEM((peer_count * shard_rows, channels), cache.dtype),
            pltpu.SemaphoreType.DMA((4,)),
            pltpu.SemaphoreType.DMA,
            pltpu.SemaphoreType.DMA,
        ],
        compiler_params=pltpu.CompilerParams(collective_id=0, has_side_effects=True),
    )(cache, lengths, slots, query)


def solution(mesh):
    return jax.shard_map(
        shards,
        mesh=mesh,
        in_specs=(
            P("grp", ("wide", "narrow"), None),
            P("grp"),
            P("grp"),
            P(("grp", "wide"), None, "narrow", None),
        ),
        out_specs=P(("grp", "wide"), None, "narrow", None),
        check_vma=False,
    )
```

```python
import functools

import jax
import jax.numpy as jnp
from jax import lax
from jax.experimental import pallas as pl
from jax.experimental.pallas import tpu as pltpu
from jax.sharding import PartitionSpec as P

LATENT_WIDTH = 512
UNROLL_LIMIT = 16

score_scale = 0.0721687836
floor_value = -1e30


def loop(count, body):
    if count <= UNROLL_LIMIT:
        for step in range(count):
            body(step)
    else:
        lax.fori_loop(0, count, lambda step, carry: (body(step), carry)[1], 0)


def kernel(
    wide_count,
    narrow_count,
    cache_hbm,
    lengths_hbm,
    slots_hbm,
    query_hbm,
    out_ref,
    cache_ref,
    lengths_ref,
    slots_ref,
    query_ref,
    outgoing,
    received,
    local_sem,
    send_sem,
    recv_sem,
):
    wide_index = lax.axis_index("wide")
    narrow_index = lax.axis_index("narrow")
    me = wide_index * narrow_count + narrow_index
    peer_count = wide_count * narrow_count
    shard_rows, request_count, channels = cache_ref.shape
    slab_rows = outgoing.shape[1]

    slots_copy = pltpu.make_async_copy(slots_hbm, slots_ref, local_sem.at[0])
    cache_copy = pltpu.make_async_copy(cache_hbm, cache_ref, local_sem.at[1])
    lengths_copy = pltpu.make_async_copy(lengths_hbm, lengths_ref, local_sem.at[2])
    query_copy = pltpu.make_async_copy(query_hbm, query_ref, local_sem.at[3])
    slots_copy.start()
    cache_copy.start()
    lengths_copy.start()
    query_copy.start()

    def peer(step):
        target = lax.rem(me + step + 1, peer_count)
        return lax.div(target, narrow_count), lax.rem(target, narrow_count)

    barrier = pltpu.get_barrier_semaphore()

    def greet(step):
        wide_peer, narrow_peer = peer(step)
        pl.semaphore_signal(
            barrier,
            inc=1,
            device_id={"wide": wide_peer, "narrow": narrow_peer},
            device_id_type=pl.DeviceIdType.MESH,
        )

    loop(peer_count - 1, greet)
    slots_copy.wait()
    cache_copy.wait()

    slot_row = slots_ref[...].reshape(1, request_count)
    shape = (request_count * slab_rows, request_count)
    row = lax.broadcasted_iota(jnp.int32, shape, 0)
    ordered = None
    for offset in range(shard_rows):
        pick = (slot_row * slab_rows + offset == row).astype(jnp.float32).astype(jnp.bfloat16)
        term = jnp.dot(pick, cache_ref[offset], preferred_element_type=jnp.float32)
        ordered = term if ordered is None else ordered + term
    outgoing[...] = ordered.reshape(outgoing.shape).astype(jnp.bfloat16)
    received[me] = outgoing[wide_index]
    pl.semaphore_wait(barrier, peer_count - 1)

    def send(step):
        wide_peer, narrow_peer = peer(step)
        pltpu.make_async_remote_copy(
            src_ref=outgoing.at[wide_peer],
            dst_ref=received.at[me],
            send_sem=send_sem,
            recv_sem=recv_sem,
            device_id={"wide": wide_peer, "narrow": narrow_peer},
            device_id_type=pl.DeviceIdType.MESH,
        ).start()

    loop(peer_count - 1, send)
    lengths_copy.wait()
    query_copy.wait()
    own_length = jnp.sum(
        jnp.where(
            slot_row == wide_index,
            lengths_ref[...].reshape(1, request_count).astype(jnp.float32),
            0.0,
        ),
        axis=1,
        keepdims=True,
    )
    _, forward_steps, head_count, _ = query_ref.shape
    score_shape = (forward_steps * head_count, peer_count * slab_rows)
    query_rows = query_ref[...].reshape(score_shape[0], channels)
    column = lax.broadcasted_iota(jnp.int32, score_shape, 1)
    offset = column % slab_rows
    place = column // slab_rows * shard_rows + offset
    token = lax.broadcasted_iota(jnp.int32, score_shape, 0) // head_count
    visible = (offset < shard_rows) & ((place - token).astype(jnp.float32) < own_length + 1.0)
    whole = received.at[pl.ds(0, peer_count - 1)]
    pltpu.make_async_copy(whole, whole, recv_sem).wait()

    keys = received[...].reshape(peer_count * slab_rows, channels)
    scores = (
        lax.dot_general(
            query_rows, keys, (((1,), (1,)), ((), ())), preferred_element_type=jnp.float32
        )
        * score_scale
    )
    scores = jnp.where(visible, scores, floor_value)
    highest = jnp.max(scores, axis=1, keepdims=True)
    weights = jnp.where(visible, jnp.exp(scores - highest), 0.0)
    weight_sum = jnp.sum(weights, axis=1, keepdims=True)
    latent_total = jnp.dot(
        weights.astype(jnp.bfloat16), keys[:, :LATENT_WIDTH], preferred_element_type=jnp.float32
    )
    out_ref[...] = (latent_total / weight_sum).astype(jnp.bfloat16).reshape(out_ref.shape)
    pltpu.make_async_copy(whole, whole, send_sem).wait()


def padded_bytes(rows, columns):
    return rows * -(-columns // 128) * 128 * 4


def shards(cache, lengths, slots, query):
    wide_count = lax.axis_size("wide")
    narrow_count = lax.axis_size("narrow")
    peer_count = wide_count * narrow_count
    request_count, shard_rows, channels = cache.shape
    _, forward_steps, head_count, _ = query.shape
    slab_rows = pl.next_power_of_2(shard_rows)
    slabs = (request_count + peer_count) * slab_rows
    limit = (4 << 20) + 4 * padded_bytes(slabs, channels)
    return pl.pallas_call(
        functools.partial(kernel, wide_count, narrow_count),
        out_shape=jax.ShapeDtypeStruct((1, forward_steps, head_count, LATENT_WIDTH), jnp.bfloat16),
        in_specs=[pl.BlockSpec(memory_space=pltpu.HBM)] * 4,
        out_specs=pl.BlockSpec(memory_space=pltpu.VMEM),
        scratch_shapes=[
            pltpu.VMEM((shard_rows, request_count, channels), cache.dtype),
            pltpu.VMEM(lengths.shape, lengths.dtype),
            pltpu.VMEM(slots.shape, slots.dtype),
            pltpu.VMEM(query.shape, query.dtype),
            pltpu.VMEM((request_count, slab_rows, channels), cache.dtype),
            pltpu.VMEM((peer_count, slab_rows, channels), cache.dtype),
            pltpu.SemaphoreType.DMA((4,)),
            pltpu.SemaphoreType.DMA,
            pltpu.SemaphoreType.DMA,
        ],
        compiler_params=pltpu.CompilerParams(
            collective_id=0, has_side_effects=True, vmem_limit_bytes=limit
        ),
    )(*[
        pltpu.with_memory_space_constraint(argument, pltpu.HBM)
        for argument in (jnp.transpose(cache, (1, 0, 2)), lengths, slots, query)
    ])


def solution(mesh):
    return jax.shard_map(
        shards,
        mesh=mesh,
        in_specs=(
            P("grp", ("wide", "narrow"), None),
            P("grp"),
            P("grp"),
            P(("grp", "wide"), None, "narrow", None),
        ),
        out_specs=P(("grp", "wide"), None, "narrow", None),
        check_vma=False,
    )
```

```python
import functools

import jax
import jax.numpy as jnp
from jax import lax
from jax.experimental import pallas as pl
from jax.experimental.pallas import tpu as pltpu
from jax.sharding import PartitionSpec as P

LATENT_WIDTH = 512
UNROLL_LIMIT = 16

score_scale = 0.0721687836
floor_value = -1e30


def loop(count, body):
    if count <= UNROLL_LIMIT:
        for step in range(count):
            body(step)
    else:
        lax.fori_loop(0, count, lambda step, carry: (body(step), carry)[1], 0)


def kernel(
    wide_count,
    narrow_count,
    cache_hbm,
    lengths_hbm,
    slots_hbm,
    query_hbm,
    out_ref,
    cache_ref,
    lengths_ref,
    slots_ref,
    query_ref,
    outgoing,
    received,
    local_sem,
    send_sem,
    recv_sem,
):
    wide_index = lax.axis_index("wide")
    narrow_index = lax.axis_index("narrow")
    me = wide_index * narrow_count + narrow_index
    peer_count = wide_count * narrow_count
    shard_rows, request_count, channels = cache_ref.shape
    slab_rows = outgoing.shape[1]

    slots_copy = pltpu.make_async_copy(slots_hbm, slots_ref, local_sem.at[0])
    cache_copy = pltpu.make_async_copy(cache_hbm, cache_ref, local_sem.at[1])
    lengths_copy = pltpu.make_async_copy(lengths_hbm, lengths_ref, local_sem.at[2])
    query_copy = pltpu.make_async_copy(query_hbm, query_ref, local_sem.at[3])
    slots_copy.start()
    cache_copy.start()
    lengths_copy.start()
    query_copy.start()

    def peer(step):
        target = step + (step >= me).astype(jnp.int32)
        return lax.div(target, narrow_count), lax.rem(target, narrow_count)

    barrier = pltpu.get_barrier_semaphore()

    def greet(step):
        wide_peer, narrow_peer = peer(step)
        pl.semaphore_signal(
            barrier,
            inc=1,
            device_id={"wide": wide_peer, "narrow": narrow_peer},
            device_id_type=pl.DeviceIdType.MESH,
        )

    loop(peer_count - 1, greet)
    slots_copy.wait()
    cache_copy.wait()

    slot_row = slots_ref[...].reshape(1, request_count)
    shape = (request_count * slab_rows, request_count)
    row = lax.broadcasted_iota(jnp.int32, shape, 0)
    ordered = None
    for offset in range(shard_rows):
        pick = (slot_row * slab_rows + offset == row).astype(jnp.float32).astype(jnp.bfloat16)
        term = jnp.dot(pick, cache_ref[offset], preferred_element_type=jnp.float32)
        ordered = term if ordered is None else ordered + term
    outgoing[...] = ordered.reshape(outgoing.shape).astype(jnp.bfloat16)
    received[me] = outgoing[wide_index]
    pl.semaphore_wait(barrier, peer_count - 1)

    def send(step):
        wide_peer, narrow_peer = peer(step)
        pltpu.make_async_remote_copy(
            src_ref=outgoing.at[wide_peer],
            dst_ref=received.at[me],
            send_sem=send_sem,
            recv_sem=recv_sem,
            device_id={"wide": wide_peer, "narrow": narrow_peer},
            device_id_type=pl.DeviceIdType.MESH,
        ).start()

    loop(peer_count - 1, send)
    lengths_copy.wait()
    query_copy.wait()
    own_length = jnp.sum(
        jnp.where(
            slot_row == wide_index,
            lengths_ref[...].reshape(1, request_count).astype(jnp.float32),
            0.0,
        ),
        axis=1,
        keepdims=True,
    )
    _, forward_steps, head_count, _ = query_ref.shape
    score_shape = (forward_steps * head_count, peer_count * slab_rows)
    query_rows = query_ref[...].reshape(score_shape[0], channels)
    column = lax.broadcasted_iota(jnp.int32, score_shape, 1)
    offset = column % slab_rows
    place = column // slab_rows * shard_rows + offset
    token = lax.broadcasted_iota(jnp.int32, score_shape, 0) // head_count
    visible = (offset < shard_rows) & ((place - token).astype(jnp.float32) < own_length + 1.0)
    whole = received.at[pl.ds(0, peer_count - 1)]
    pltpu.make_async_copy(whole, whole, recv_sem).wait()

    keys = received[...].reshape(peer_count * slab_rows, channels)
    scores = (
        lax.dot_general(
            query_rows, keys, (((1,), (1,)), ((), ())), preferred_element_type=jnp.float32
        )
        * score_scale
    )
    scores = jnp.where(visible, scores, floor_value)
    highest = jnp.max(scores, axis=1, keepdims=True)
    weights = jnp.where(visible, jnp.exp(scores - highest), 0.0)
    weight_sum = jnp.sum(weights, axis=1, keepdims=True)
    latent_total = jnp.dot(
        weights.astype(jnp.bfloat16), keys[:, :LATENT_WIDTH], preferred_element_type=jnp.float32
    )
    out_ref[...] = (latent_total / weight_sum).astype(jnp.bfloat16).reshape(out_ref.shape)
    pltpu.make_async_copy(whole, whole, send_sem).wait()


def padded_bytes(rows, columns):
    return rows * -(-columns // 128) * 128 * 4


def shards(cache, lengths, slots, query):
    wide_count = lax.axis_size("wide")
    narrow_count = lax.axis_size("narrow")
    peer_count = wide_count * narrow_count
    request_count, shard_rows, channels = cache.shape
    _, forward_steps, head_count, _ = query.shape
    slab_rows = pl.next_power_of_2(shard_rows)
    slabs = (request_count + peer_count) * slab_rows
    limit = (4 << 20) + 4 * padded_bytes(slabs, channels)
    return pl.pallas_call(
        functools.partial(kernel, wide_count, narrow_count),
        out_shape=jax.ShapeDtypeStruct((1, forward_steps, head_count, LATENT_WIDTH), jnp.bfloat16),
        in_specs=[pl.BlockSpec(memory_space=pltpu.HBM)] * 4,
        out_specs=pl.BlockSpec(memory_space=pltpu.VMEM),
        scratch_shapes=[
            pltpu.VMEM((shard_rows, request_count, channels), cache.dtype),
            pltpu.VMEM(lengths.shape, lengths.dtype),
            pltpu.VMEM(slots.shape, slots.dtype),
            pltpu.VMEM(query.shape, query.dtype),
            pltpu.VMEM((request_count, slab_rows, channels), cache.dtype),
            pltpu.VMEM((peer_count, slab_rows, channels), cache.dtype),
            pltpu.SemaphoreType.DMA((4,)),
            pltpu.SemaphoreType.DMA,
            pltpu.SemaphoreType.DMA,
        ],
        compiler_params=pltpu.CompilerParams(
            collective_id=0, has_side_effects=True, vmem_limit_bytes=limit
        ),
    )(*[
        pltpu.with_memory_space_constraint(argument, pltpu.HBM)
        for argument in (jnp.transpose(cache, (1, 0, 2)), lengths, slots, query)
    ])


def solution(mesh):
    return jax.shard_map(
        shards,
        mesh=mesh,
        in_specs=(
            P("grp", ("wide", "narrow"), None),
            P("grp"),
            P("grp"),
            P(("grp", "wide"), None, "narrow", None),
        ),
        out_specs=P(("grp", "wide"), None, "narrow", None),
        check_vma=False,
    )
```

```python
import functools

import jax
import jax.numpy as jnp
from jax import lax
from jax.experimental import pallas as pl
from jax.experimental.pallas import tpu as pltpu
from jax.sharding import PartitionSpec as P

LATENT_WIDTH = 512
UNROLL_LIMIT = 16

score_scale = 0.0721687836
floor_value = -1e30


def loop(count, body):
    if count <= UNROLL_LIMIT:
        for step in range(count):
            body(step)
    else:
        lax.fori_loop(0, count, lambda step, carry: (body(step), carry)[1], 0)


def kernel(
    wide_count,
    narrow_count,
    cache_hbm,
    lengths_hbm,
    slots_hbm,
    query_hbm,
    out_ref,
    cache_ref,
    lengths_ref,
    slots_ref,
    query_ref,
    outgoing,
    received,
    local_sem,
    send_sem,
    recv_sem,
):
    wide_index = lax.axis_index("wide")
    narrow_index = lax.axis_index("narrow")
    me = wide_index * narrow_count + narrow_index
    peer_count = wide_count * narrow_count
    shard_rows, request_count, channels = cache_ref.shape
    slab_rows = outgoing.shape[1]

    slots_copy = pltpu.make_async_copy(slots_hbm, slots_ref, local_sem.at[0])
    cache_copy = pltpu.make_async_copy(cache_hbm, cache_ref, local_sem.at[1])
    lengths_copy = pltpu.make_async_copy(lengths_hbm, lengths_ref, local_sem.at[2])
    query_copy = pltpu.make_async_copy(query_hbm, query_ref, local_sem.at[3])
    slots_copy.start()
    cache_copy.start()
    lengths_copy.start()
    query_copy.start()

    def peer(step):
        target = lax.rem(me + step + 1, peer_count)
        return lax.div(target, narrow_count), lax.rem(target, narrow_count)

    barrier = pltpu.get_barrier_semaphore()

    def greet(step):
        wide_peer, narrow_peer = peer(step)
        pl.semaphore_signal(
            barrier,
            inc=1,
            device_id={"wide": wide_peer, "narrow": narrow_peer},
            device_id_type=pl.DeviceIdType.MESH,
        )

    loop(peer_count - 1, greet)
    slots_copy.wait()
    cache_copy.wait()

    slot_row = slots_ref[...].reshape(1, request_count)
    shape = (request_count * slab_rows, request_count)
    row = lax.broadcasted_iota(jnp.int32, shape, 0)
    ordered = None
    for offset in range(shard_rows):
        pick = (slot_row * slab_rows + offset == row).astype(jnp.float32).astype(jnp.bfloat16)
        term = jnp.dot(pick, cache_ref[offset], preferred_element_type=jnp.float32)
        ordered = term if ordered is None else ordered + term
    outgoing[...] = ordered.reshape(outgoing.shape).astype(jnp.bfloat16)
    pl.semaphore_wait(barrier, peer_count - 1)

    def send(step):
        wide_peer, narrow_peer = peer(step)
        pltpu.make_async_remote_copy(
            src_ref=outgoing.at[wide_peer],
            dst_ref=received.at[me],
            send_sem=send_sem,
            recv_sem=recv_sem,
            device_id={"wide": wide_peer, "narrow": narrow_peer},
            device_id_type=pl.DeviceIdType.MESH,
        ).start()

    loop(peer_count - 1, send)
    received[me] = outgoing[wide_index]
    lengths_copy.wait()
    query_copy.wait()
    own_length = jnp.sum(
        jnp.where(
            slot_row == wide_index,
            lengths_ref[...].reshape(1, request_count).astype(jnp.float32),
            0.0,
        ),
        axis=1,
        keepdims=True,
    )
    _, forward_steps, head_count, _ = query_ref.shape
    score_shape = (forward_steps * head_count, peer_count * slab_rows)
    query_rows = query_ref[...].reshape(score_shape[0], channels)
    column = lax.broadcasted_iota(jnp.int32, score_shape, 1)
    offset = column % slab_rows
    place = column // slab_rows * shard_rows + offset
    token = lax.broadcasted_iota(jnp.int32, score_shape, 0) // head_count
    visible = (offset < shard_rows) & ((place - token).astype(jnp.float32) < own_length + 1.0)
    whole = received.at[pl.ds(0, peer_count - 1)]
    pltpu.make_async_copy(whole, whole, recv_sem).wait()

    keys = received[...].reshape(peer_count * slab_rows, channels)
    scores = (
        lax.dot_general(
            query_rows, keys, (((1,), (1,)), ((), ())), preferred_element_type=jnp.float32
        )
        * score_scale
    )
    scores = jnp.where(visible, scores, floor_value)
    highest = jnp.max(scores, axis=1, keepdims=True)
    weights = jnp.where(visible, jnp.exp(scores - highest), 0.0)
    weight_sum = jnp.sum(weights, axis=1, keepdims=True)
    latent_total = jnp.dot(
        weights.astype(jnp.bfloat16), keys[:, :LATENT_WIDTH], preferred_element_type=jnp.float32
    )
    out_ref[...] = (latent_total / weight_sum).astype(jnp.bfloat16).reshape(out_ref.shape)
    pltpu.make_async_copy(whole, whole, send_sem).wait()


def padded_bytes(rows, columns):
    return rows * -(-columns // 128) * 128 * 4


def shards(cache, lengths, slots, query):
    wide_count = lax.axis_size("wide")
    narrow_count = lax.axis_size("narrow")
    peer_count = wide_count * narrow_count
    request_count, shard_rows, channels = cache.shape
    _, forward_steps, head_count, _ = query.shape
    slab_rows = pl.next_power_of_2(shard_rows)
    slabs = (request_count + peer_count) * slab_rows
    limit = (4 << 20) + 4 * padded_bytes(slabs, channels)
    return pl.pallas_call(
        functools.partial(kernel, wide_count, narrow_count),
        out_shape=jax.ShapeDtypeStruct((1, forward_steps, head_count, LATENT_WIDTH), jnp.bfloat16),
        in_specs=[pl.BlockSpec(memory_space=pltpu.HBM)] * 4,
        out_specs=pl.BlockSpec(memory_space=pltpu.VMEM),
        scratch_shapes=[
            pltpu.VMEM((shard_rows, request_count, channels), cache.dtype),
            pltpu.VMEM(lengths.shape, lengths.dtype),
            pltpu.VMEM(slots.shape, slots.dtype),
            pltpu.VMEM(query.shape, query.dtype),
            pltpu.VMEM((request_count, slab_rows, channels), cache.dtype),
            pltpu.VMEM((peer_count, slab_rows, channels), cache.dtype),
            pltpu.SemaphoreType.DMA((4,)),
            pltpu.SemaphoreType.DMA,
            pltpu.SemaphoreType.DMA,
        ],
        compiler_params=pltpu.CompilerParams(
            collective_id=0, has_side_effects=True, vmem_limit_bytes=limit
        ),
    )(*[
        pltpu.with_memory_space_constraint(argument, pltpu.HBM)
        for argument in (jnp.transpose(cache, (1, 0, 2)), lengths, slots, query)
    ])


def solution(mesh):
    return jax.shard_map(
        shards,
        mesh=mesh,
        in_specs=(
            P("grp", ("wide", "narrow"), None),
            P("grp"),
            P("grp"),
            P(("grp", "wide"), None, "narrow", None),
        ),
        out_specs=P(("grp", "wide"), None, "narrow", None),
        check_vma=False,
    )
```
